32 devices in a mesh: pair: 4 (over y, x), side: 2 (over core), blk: 4 (over z).
Axes of the slice: x: 2, y: 2, z: 4, core: 2. Of those that a mesh axis runs over, the one named last changes fastest.
Arguments:
- intersect: float32 [4096, 768], P(('pair', 'side', 'blk')), parts along dimension 0, may hold values from -0.1 to 1.7, as said below
- half_factors: float32 [4096, 384], P(('pair', 'side', 'blk')), parts along dimension 0, may hold values from -0.03 to 1.35, as said below
- z_pattern: int32 [32, 6], P(('pair', 'side', 'blk')), parts along dimension 0, may hold values 0 or 1
Outputs:
- refined_factor: float32 [4096, 768], P(('pair', 'side', 'blk')), parts along dimension 0
The draws below stay inside these ranges and needn't reach their ends.
There are 4 independent parts, one for each index of `pair`. The reference program is written for one: setup_inputs(seed, part) draws one part's arguments, and reference() takes and returns one part's arrays. A program takes and returns all parts, laid end to end along the dimension named above; each array names one. Nothing has to cross between parts.
Inputs may be any that keep to these rules, and one draw needn't show every extreme that they name: As a whole windowed matrix, intersect is symmetric: S[a, b] = S[b, a]. `half_factors`: entries of the other half and outside the grid of blocks are absent or zero. `z_pattern`: 1 keeps a tile of the factor, 0 drops it; diagonal tiles are kept whatever it says.
All inputs are finite; a program needn't handle non-finite values. No bound on the sum of `z_pattern` on one device may be relied on, other than what follows from the above.
Results may differ from the reference program's by a relative error of at most 0.0001.
Values sent between devices are 32-bit elements; how exact they have to be, the bound alone decides.
No kernel may reach another device: no remote copies, remote signals or barrier semaphores. Data moves between devices by JAX's collectives and lax.ppermute only.
A program may use at most 64 MiB of HBM per device.

```python
import jax
import jax.numpy as jnp
from jax import lax

TILE = 128
TILES_DEV = 1
ITERS = 2
TILE_ROWS = 8
N_BLK = 4


def diag_values(key):
    rows = TILE * TILES_DEV
    draw_key = jax.random.fold_in(key, 11)
    fraction = jax.random.uniform(draw_key, (2, N_BLK, rows), jnp.float32)
    return 0.7 * jnp.exp(fraction * jnp.log(1.5 / 0.7))


def block_inside(blocks):
    column = jnp.arange(blocks)[:, None] + jnp.arange(3)[None, :] - 1
    return ((column >= 0) & (column < blocks)).astype(jnp.float32)


def window_transpose(field):
    empty = jnp.zeros_like(field[:, :1, :, 0])
    pieces = []
    for slot in range(3):
        source = field[:, :, :, 2 - slot]
        if slot == 2:
            source = jnp.concatenate((source[:, 1:], empty), axis=1)
        if slot == 0:
            source = jnp.concatenate((empty, source[:, :-1]), axis=1)
        pieces.append(jnp.transpose(source, (3, 1, 4, 0, 2)))
    return jnp.stack(pieces, axis=3)


def draw_intersect(key, part):
    rows = TILE * TILES_DEV
    blocks = N_BLK
    shape = (2, blocks, rows, 3, 2, rows)
    sigma = 0.012
    noise_key = jax.random.fold_in(key, 3)
    raw = jnp.clip(jax.random.normal(noise_key, shape, jnp.float32), -6.0, 6.0) * sigma
    tile_key = jax.random.fold_in(key, 5)
    present = jax.random.bernoulli(tile_key, 0.75, (2, blocks, TILES_DEV, 3, 2, TILES_DEV)).astype(jnp.float32)
    present = jnp.repeat(jnp.repeat(present, TILE, axis=2), TILE, axis=5)
    inside = block_inside(blocks)[None, :, None, :, None, None]
    coupling = raw * present * inside
    symmetric = 0.5 * (coupling + window_transpose(coupling))
    eye_side = jnp.eye(2, dtype=jnp.float32)
    eye_rows = jnp.eye(rows, dtype=jnp.float32)
    middle = (jnp.arange(3) == 1).astype(jnp.float32)
    diagonal = diag_values(key)[:, :, :, None, None, None] * eye_side[:, None, None, None, :, None] * eye_rows[None, None, :, None, None, :] * middle[None, None, None, :, None, None]
    return (symmetric + diagonal).reshape(2 * blocks * rows, 6 * rows)


def draw_half_factors(key, part):
    rows = TILE * TILES_DEV
    blocks = N_BLK
    shape = (2, blocks, rows, 3, rows)
    sigma = 0.004
    noise_key = jax.random.fold_in(key, 17)
    raw = jnp.clip(jax.random.normal(noise_key, shape, jnp.float32), -6.0, 6.0) * sigma
    inside = block_inside(blocks)[None, :, None, :, None]
    eye_rows = jnp.eye(rows, dtype=jnp.float32)
    middle = (jnp.arange(3) == 1).astype(jnp.float32)
    scales = 1.0 / jnp.sqrt(diag_values(key))
    diagonal = scales[:, :, :, None, None] * eye_rows[None, None, :, None, :] * middle[None, None, None, :, None]
    return (raw * inside + diagonal).reshape(2 * blocks * rows, 3 * rows)


def set_ends(array, rng, low, top_value):
    index_at = [jax.random.randint(jax.random.fold_in(rng, axis), (), 0, length) for axis, length in enumerate(array.shape)]
    main_axis = array.shape.index(max(array.shape))
    next_to = index_at[:main_axis] + [(index_at[main_axis] + 1) % array.shape[main_axis]] + index_at[main_axis + 1:]
    return array.at[tuple(index_at)].set(low).at[tuple(next_to)].set(top_value)


def setup_inputs(seed: int = 0, part: int = 0) -> dict:
    seeds = jax.random.split(jax.random.key(seed), 4)
    own_keys = jax.random.split(jax.random.fold_in(seeds[3], part), 4)
    return {
        "intersect": draw_intersect(jax.random.fold_in(jax.random.fold_in(seeds[3], part), 71), part),
        "half_factors": draw_half_factors(jax.random.fold_in(jax.random.fold_in(seeds[3], part), 71), part),
        "z_pattern": set_ends((jax.random.randint(own_keys[2], (TILE_ROWS, 6 * TILES_DEV), 0, 4) < 3).astype(jnp.int32), jax.random.fold_in(own_keys[2], 1), 0, 1),
    }


def shift_blocks(field, offset):
    empty = jnp.zeros_like(field[:, :1])
    if offset == 1:
        return jnp.concatenate((field[:, 1:], empty), axis=1)
    if offset == -1:
        return jnp.concatenate((empty, field[:, :-1]), axis=1)
    return field


def shift_slots(term, slot):
    empty = jnp.zeros_like(term[:, :, :, :1])
    if slot == 0:
        return jnp.concatenate((term[:, :, :, 1:], empty), axis=3)
    if slot == 2:
        return jnp.concatenate((empty, term[:, :, :, :2]), axis=3)
    return term


def window_product(left, right):
    total = jnp.zeros_like(right)
    for slot in range(3):
        nearby = shift_blocks(right, slot - 1)
        term = jnp.einsum("sbixk,xbkdyj->sbidyj", left[:, :, :, slot], nearby, precision=lax.Precision.HIGHEST)
        total = total + shift_slots(term, slot)
    return total


def window_cross(factor, image):
    total = jnp.zeros_like(image)
    for slot in range(3):
        near_factor = shift_blocks(factor, slot - 1)
        near_image = shift_blocks(image, slot - 1)
        term = jnp.einsum("xbksi,xbkdyj->sbidyj", near_factor[:, :, :, 2 - slot], near_image, precision=lax.Precision.HIGHEST)
        total = total + shift_slots(term, slot)
    return total


def reference(intersect, half_factors, z_pattern):
    blocks = N_BLK
    rows = intersect.shape[1] // 6
    tiles = z_pattern.shape[1] // 6
    tile = rows // tiles
    intersect_win = intersect.reshape(2, blocks, rows, 3, 2, rows)
    half_win = half_factors.reshape(2, blocks, rows, 3, rows)
    eye_side = jnp.eye(2, dtype=jnp.float32)
    eye_rows = jnp.eye(rows, dtype=jnp.float32)
    middle = (jnp.arange(3) == 1).astype(jnp.float32)
    identity = eye_side[:, None, None, None, :, None] * eye_rows[None, None, :, None, None, :] * middle[None, None, None, :, None, None]
    grid = z_pattern.reshape(2, blocks, tiles, 3, 2, tiles)
    halves = jnp.arange(2)
    tile_ids = jnp.arange(tiles)
    diagonal = (halves[:, None, None, None, None, None] == halves[None, None, None, None, :, None]) & (tile_ids[None, None, :, None, None, None] == tile_ids[None, None, None, None, None, :]) & (jnp.arange(3)[None, None, None, :, None, None] == 1)
    kept = jnp.maximum(grid, diagonal.astype(jnp.int32)).astype(jnp.float32)
    wide = jnp.broadcast_to(kept[:, :, :, None, :, :, :, None], (2, blocks, tiles, tile, 3, 2, tiles, tile))
    keep = wide.reshape(2, blocks, rows, 3, 2, rows)
    factor = half_win[:, :, :, :, None, :] * eye_side[:, None, None, None, :, None]
    for step in range(ITERS):
        image = window_product(intersect_win, factor)
        delta = identity - window_cross(factor, image)
        first = window_product(factor, delta)
        second = window_product(first, delta)
        factor = keep * (factor + 0.5 * first + 0.375 * second)
    return factor.reshape(2 * blocks * rows, 6 * rows)
```

```python
import jax
import jax.numpy as jnp
from jax import lax
from jax.experimental import pallas as pl
from jax.experimental.pallas import tpu as pltpu
from jax.sharding import PartitionSpec as P

ITERS = 2
BF = jnp.bfloat16
F32 = jnp.float32


def halves_of(value):
    high = value.astype(BF)
    low = (value - high.astype(F32)).astype(BF)
    return high, low


def product(left, right, dims):
    (lh, ll), (rh, rl) = left, right

    def dot(a, b):
        return lax.dot_general(a, b, (dims, ((), ())), preferred_element_type=F32)

    return dot(lh, rh) + (dot(lh, rl) + dot(ll, rh))


def nn(left, right):
    return product(left, right, ((1,), (0,)))


def tn(left, right):
    return product(left, right, ((0,), (0,)))


def ordered(side, own, other):
    return jnp.where(side == 0, own, other), jnp.where(side == 0, other, own)


def near(place, own, other):
    side, blk, last = place
    below, above = ordered(side, own, other)
    return jnp.where(blk > 0, below, 0.0), jnp.where(blk < last, above, 0.0)


def block_diag(top, bottom):
    zero = jnp.zeros_like(top)
    return jnp.concatenate(
        [jnp.concatenate([top, zero], axis=1), jnp.concatenate([zero, bottom], axis=1)], axis=0
    )


def place_of(ref):
    return ref[0], ref[1], ref[2]


def wide_row(side, own, other, rows):
    top, bottom = ordered(side, own, other)
    return [block_diag(top[:, e * rows:(e + 1) * rows], bottom[:, e * rows:(e + 1) * rows]) for e in range(3)]


def delta_column(s_row, s_below, s_above, z_row, z_below, z_above, width):
    s0, s1, s2 = [halves_of(v) for v in s_row]
    sb, sa = halves_of(s_below), halves_of(s_above)
    z0, z1, z2 = [halves_of(v) for v in z_row]
    zb0, zb1 = [halves_of(v) for v in z_below]
    za0, za1 = [halves_of(v) for v in z_above]
    i0 = halves_of(nn(sb, zb1) + tn(s0, z1))
    i1 = halves_of(nn(s0, zb1) + nn(s1, z1) + nn(s2, za0))
    i2 = halves_of(tn(s2, z1) + nn(sa, za0))
    d0 = -(tn(zb0, i0) + tn(z0, i1))
    row_ids = lax.broadcasted_iota(jnp.int32, (width, width), 0)
    col_ids = lax.broadcasted_iota(jnp.int32, (width, width), 1)
    eye = (row_ids == col_ids).astype(F32)
    d1 = eye - (tn(zb1, i0) + tn(z1, i1) + tn(za0, i2))
    d2 = -(tn(z2, i1) + tn(za1, i2))
    return d0, d1, d2


def write_delta(side, deltas, col_ref, pay_ref, width):
    for e in range(3):
        col_ref[e * width:(e + 1) * width, :] = deltas[e]
    for e in range(2):
        pay_ref[e * width:(e + 1) * width, :] = jnp.where(side == 0, deltas[e + 1], deltas[e])


def start_kernel(place, s_own, s_oth, h_own, h_oth, pay_ref):
    side = place[0]
    rows = s_own.shape[0]
    width = 2 * rows
    top, bottom = ordered(side, s_own[:, width:2 * width], s_oth[:, width:2 * width])
    pay_ref[:rows, :width] = top
    pay_ref[rows:, :width] = bottom
    pick = lambda ref: jnp.where(side == 0, ref[:, rows:3 * rows], ref[:, :2 * rows])
    top, bottom = ordered(side, pick(h_own), pick(h_oth))
    pay_ref[:rows, width:] = top
    pay_ref[rows:, width:] = bottom


def first_delta_kernel(place, s_own, s_oth, h_own, h_oth, r_own, r_oth, col_ref, pay_ref):
    where = place_of(place)
    side = where[0]
    rows = s_own.shape[0]
    width = 2 * rows
    s_all = jnp.concatenate(ordered(side, s_own[...], s_oth[...]), axis=0)
    s_row = [s_all[:, e * width:(e + 1) * width] for e in range(3)]
    z_row = wide_row(side, h_own[...], h_oth[...], rows)
    below, above = near(where, r_own[...], r_oth[...])

    def split(part):
        cells = part[:, width:]
        return [block_diag(cells[:rows, e * rows:(e + 1) * rows], cells[rows:, e * rows:(e + 1) * rows]) for e in range(2)]

    deltas = delta_column(s_row, below[:, :width], above[:, :width], z_row, split(below), split(above), width)
    write_delta(side, deltas, col_ref, pay_ref, width)


def next_delta_kernel(place, s_own, s_oth, s_rown, s_roth, z_ref, r_own, r_oth, col_ref, pay_ref):
    where = place_of(place)
    side = where[0]
    rows = s_own.shape[0]
    width = 2 * rows
    s_all = jnp.concatenate(ordered(side, s_own[...], s_oth[...]), axis=0)
    s_row = [s_all[:, e * width:(e + 1) * width] for e in range(3)]
    z_row = [z_ref[:, e * width:(e + 1) * width] for e in range(3)]
    s_below, s_above = near(where, s_rown[:, :width], s_roth[:, :width])
    below, above = near(where, r_own[...], r_oth[...])
    split = lambda part: [part[:, :width], part[:, width:]]
    deltas = delta_column(s_row, s_below, s_above, z_row, split(below), split(above), width)
    write_delta(side, deltas, col_ref, pay_ref, width)


def factor_rows(z_row, col_ref, below, above, width):
    z0, z1, z2 = [halves_of(v) for v in z_row]
    d = [halves_of(col_ref[e * width:(e + 1) * width, :]) for e in range(3)]
    b0, b1 = halves_of(below[:width]), halves_of(below[width:])
    a0, a1 = halves_of(above[:width]), halves_of(above[width:])

    def apply(x0, x1, x2):
        return (
            nn(x0, b0) + nn(x1, b1),
            nn(x0, d[0]) + nn(x1, d[1]) + nn(x2, d[2]),
            nn(x1, a0) + nn(x2, a1),
        )

    first = apply(z0, z1, z2)
    second = apply(*[halves_of(v) for v in first])
    return [z_row[e] + 0.5 * first[e] + 0.375 * second[e] for e in range(3)]


def kept(values, pattern, half, rows):
    count = pattern.shape[0]
    tile = rows // count
    bands = []
    for i in range(count):
        cells = []
        for q in range(6 * count):
            flag = jnp.logical_or(pattern[i, q] == 1, (2 + half) * count + i == q)
            cell = values[i * tile:(i + 1) * tile, q * tile:(q + 1) * tile]
            cells.append(jnp.where(flag, 1.0, 0.0) * cell)
        bands.append(jnp.concatenate(cells, axis=1))
    return bands[0] if count == 1 else jnp.concatenate(bands, axis=0)


def first_factor_kernel(place, pat_own, pat_oth, h_own, h_oth, col_ref, r_own, r_oth, z_ref, pay_ref):
    where = place_of(place)
    side = where[0]
    rows = h_own.shape[0]
    width = 2 * rows
    z_row = wide_row(side, h_own[...], h_oth[...], rows)
    below, above = near(where, r_own[...], r_oth[...])
    full = jnp.concatenate(factor_rows(z_row, col_ref, below, above, width), axis=1)
    own_rows = jnp.where(side == 0, full[:rows], full[rows:])
    oth_rows = jnp.where(side == 0, full[rows:], full[:rows])
    own_rows = kept(own_rows, pat_own, side, rows)
    oth_rows = kept(oth_rows, pat_oth, 1 - side, rows)
    top, bottom = ordered(side, own_rows, oth_rows)
    z_ref[:rows, :] = top
    z_ref[rows:, :] = bottom
    pay_ref[:rows, :] = jnp.where(side == 0, top[:, width:], top[:, :2 * width])
    pay_ref[rows:, :] = jnp.where(side == 0, bottom[:, width:], bottom[:, :2 * width])


def last_factor_kernel(place, pat_own, z_ref, col_ref, r_own, r_oth, out_ref):
    where = place_of(place)
    side = where[0]
    rows = out_ref.shape[0]
    width = 2 * rows
    mine = jnp.where(side == 0, z_ref[:rows, :], z_ref[rows:, :])
    z_row = [mine[:, e * width:(e + 1) * width] for e in range(3)]
    below, above = near(where, r_own[...], r_oth[...])
    full = jnp.concatenate(factor_rows(z_row, col_ref, below, above, width), axis=1)
    out_ref[...] = kept(full, pat_own, side, rows)


def call(kernel, outs, scalars, arrays):
    smem = pl.BlockSpec(memory_space=pltpu.SMEM)
    vmem = pl.BlockSpec(memory_space=pltpu.VMEM)
    shapes = [jax.ShapeDtypeStruct(s, F32) for s in outs]
    many = len(shapes) > 1
    return pl.pallas_call(
        kernel,
        out_shape=shapes if many else shapes[0],
        in_specs=[smem] * len(scalars) + [vmem] * len(arrays),
        out_specs=[vmem] * len(shapes) if many else vmem,
    )(*scalars, *arrays)


def per_device(intersect, half_factors, z_pattern):
    rows = intersect.shape[0]
    width = 2 * rows
    count = lax.axis_size("blk")
    side = lax.axis_index("side")
    place = jnp.stack([side, lax.axis_index("blk"), jnp.int32(count - 1)]).astype(jnp.int32)
    last = count - 1
    cycle = [(i, i + 1) for i in range(last)] + [(last, count + last)]
    cycle += [(count + i + 1, count + i) for i in range(last)] + [(count, 0)]

    def swap(value):
        return lax.ppermute(value, "side", [(0, 1), (1, 0)])

    def exchange(payload):
        got = lax.ppermute(payload, ("side", "blk"), cycle)
        return got, swap(got)

    s_oth, h_oth, p_oth = swap(intersect), swap(half_factors), swap(z_pattern)
    inputs = [intersect, s_oth, half_factors, h_oth]
    payload = call(start_kernel, [(width, 2 * width)], [place], inputs)
    near_in = exchange(payload)
    column, payload = call(first_delta_kernel, [(3 * width, width), (2 * width, width)], [place], inputs + list(near_in))
    near_delta = exchange(payload)
    for step in range(ITERS - 1):
        if step == 0:
            factor, payload = call(
                first_factor_kernel, [(width, 3 * width), (width, 2 * width)], [place, z_pattern, p_oth],
                [half_factors, h_oth, column, *near_delta])
        near_factor = exchange(payload)
        column, payload = call(
            next_delta_kernel, [(3 * width, width), (2 * width, width)], [place],
            [intersect, s_oth, *near_in, factor, *near_factor])
        near_delta = exchange(payload)
    return call(last_factor_kernel, [(rows, 3 * width)], [place, z_pattern], [factor, column, *near_delta])


def solution(mesh):
    spec = P(("pair", "side", "blk"), None)
    return jax.shard_map(
        per_device,
        mesh=mesh,
        in_specs=(spec, spec, spec),
        out_specs=spec,
        check_vma=False,
    )
```

```python
import jax
import jax.numpy as jnp
from jax import lax
from jax.experimental import pallas as pl
from jax.experimental.pallas import tpu as pltpu
from jax.sharding import PartitionSpec as P


ITERS = 2
BF = jnp.bfloat16
F32 = jnp.float32


def halves_of(value):
    high = value.astype(BF)
    low = (value - high.astype(F32)).astype(BF)
    return high, low


def product(left, right, dims):
    (lh, ll), (rh, rl) = left, right

    def dot(a, b):
        return lax.dot_general(a, b, (dims, ((), ())), preferred_element_type=F32)

    return dot(lh, rh) + (dot(lh, rl) + dot(ll, rh))


def nn(left, right):
    return product(left, right, ((1,), (0,)))


def tn(left, right):
    return product(left, right, ((0,), (0,)))


def ordered(side, own, other):
    return jnp.where(side == 0, own, other), jnp.where(side == 0, other, own)


def block_diag(top, bottom):
    zero = jnp.zeros_like(top)
    return jnp.concatenate(
        [jnp.concatenate([top, zero], axis=1), jnp.concatenate([zero, bottom], axis=1)], axis=0
    )


def oriented(side, row, width):
    first, middle, final = [row[:, e * width:(e + 1) * width] for e in range(3)]
    near, far = ordered(side, first, final)
    return near, middle, far


def start_kernel(place, pattern, s_own, s_oth, h_own, h_oth, pay_ref):
    side = place[0]
    rows = s_own.shape[0]
    width = 2 * rows
    top, bottom = ordered(side, s_own[:, width:2 * width], s_oth[:, width:2 * width])
    pay_ref[:rows, :width] = top
    pay_ref[rows:, :width] = bottom
    top, bottom = ordered(side, h_own[...], h_oth[...])
    for part, at in ((top, 0), (bottom, rows)):
        _, middle, far = oriented(side, part, rows)
        pay_ref[at:at + rows, width:width + rows] = middle
        pay_ref[at:at + rows, width + rows:] = far


def image_local(s_row, z_mid, outs):
    near, middle, far = [halves_of(v) for v in s_row]
    z = halves_of(z_mid)
    outs[0][...] = tn(near, z)
    outs[1][...] = nn(middle, z)
    outs[2][...] = tn(far, z)


def first_local_kernel(place, s_own, s_oth, h_own, h_oth, sn, sm, sf, zn, zm, zf, tn_, tm, tf):
    side = place[0]
    rows = s_own.shape[0]
    width = 2 * rows
    s_all = jnp.concatenate(ordered(side, s_own[...], s_oth[...]), axis=0)
    s_row = oriented(side, s_all, width)
    top, bottom = ordered(side, h_own[...], h_oth[...])
    z_row = [block_diag(a, b) for a, b in zip(oriented(side, top, rows), oriented(side, bottom, rows))]
    for ref, v in zip((sn, sm, sf, zn, zm, zf), [*s_row, *z_row]):
        ref[...] = v
    image_local(s_row, z_row[1], (tn_, tm, tf))


def next_local_kernel(place, sn, sm, sf, zm, tn_, tm, tf):
    image_local((sn[...], sm[...], sf[...]), zm[...], (tn_, tm, tf))


def factor_parts(got_ref, keep, split):
    got = jnp.where(keep == 1, got_ref[...], 0.0)
    width = got.shape[0]
    if not split:
        return got[:, :width], got[:, width:]
    rows = width // 2
    cells = got[:, width:]
    return [block_diag(cells[:rows, e * rows:(e + 1) * rows], cells[rows:, e * rows:(e + 1) * rows]) for e in range(2)]


def overlap_part(got_ref, keep, width):
    return halves_of(jnp.where(keep == 1, got_ref[:, :width], 0.0))


def near_image_kernel(split):
    def kernel(place, s_got, z_got, sn, t_near, t_mid, mid_ref, e_near, e_mid):
        width = t_near.shape[0]
        diag, off = [halves_of(v) for v in factor_parts(z_got, place[1], split)]
        image_near = halves_of(nn(overlap_part(s_got, place[1], width), off) + t_near[...])
        mid_ref[...] = t_mid[...] + nn(halves_of(sn[...]), off)
        e_near[...] = tn(diag, image_near)
        e_mid[...] = tn(off, image_near)

    return kernel


def far_image_kernel(split):
    def kernel(place, s_got, z_got, sf, zm, zf, t_far, mid_part, e_mid, mid_ref, pay_ref):
        width = t_far.shape[0]
        diag, off = [halves_of(v) for v in factor_parts(z_got, place[2], split)]
        middle = mid_part[...] + nn(halves_of(sf[...]), off)
        mid_ref[...] = middle
        middle = halves_of(middle)
        image_far = halves_of(nn(overlap_part(s_got, place[2], width), off) + t_far[...])
        row_ids = lax.broadcasted_iota(jnp.int32, (width, width), 0)
        col_ids = lax.broadcasted_iota(jnp.int32, (width, width), 1)
        eye = (row_ids == col_ids).astype(F32)
        pay_ref[:width] = eye - (e_mid[...] + tn(halves_of(zm[...]), middle) + tn(off, image_far))
        pay_ref[width:] = -(tn(halves_of(zf[...]), middle) + tn(diag, image_far))

    return kernel


def own_rows(ref, side, rows):
    if ref.shape[0] == rows:
        return ref[...]
    return jnp.where(side == 0, ref[:rows, :], ref[rows:, :])


def mid_first_kernel(place, zn, zm, zf, e_near, mid, pay, d_near, first_ref, part_ref):
    side = place[0]
    width = zn.shape[0]
    rows = first_ref.shape[0]
    d_new = -(e_near[...] + tn(halves_of(zn[...]), halves_of(mid[...])))
    d_near[...] = d_new
    d_mid = halves_of(pay[:width])
    first = nn(halves_of(own_rows(zn, side, rows)), halves_of(d_new))
    first += nn(halves_of(own_rows(zm, side, rows)), d_mid)
    first += nn(halves_of(own_rows(zf, side, rows)), halves_of(pay[width:]))
    first_ref[...] = first
    part_ref[...] = nn(halves_of(first), d_mid)


def kept(values, pats, side, slot, rows):
    count = pats[0].shape[0]
    tile = rows // count
    both = values.shape[0] != rows
    bands = []
    for f in range(2 if both else 1):
        half = f if both else side
        for i in range(count):
            cells = []
            for q in range(2 * count):
                at = slot * 2 * count + q
                bit = jnp.where(side == f, pats[0][i, at], pats[1][i, at]) if both else pats[0][i, at]
                flag = jnp.logical_or(bit == 1, (2 + half) * count + i == at)
                top = (f * count + i) * tile
                cell = values[top:top + tile, q * tile:(q + 1) * tile]
                cells.append(jnp.where(flag, 1.0, 0.0) * cell)
            bands.append(jnp.concatenate(cells, axis=1))
    return jnp.concatenate(bands, axis=0) if len(bands) > 1 else bands[0]


def side_products(got, keep, z_side, z_mid, first, width):
    got = jnp.where(keep == 1, got, 0.0)
    diag, off = halves_of(got[:width]), halves_of(got[width:])
    outer = nn(halves_of(z_side), diag) + nn(halves_of(z_mid), off)
    split = halves_of(outer)
    second = nn(split, diag) + nn(halves_of(first), off)
    return outer, split, second


def near_factor_kernel(place, *refs):
    pats, (got, zn, zm, first, part, d_near, new_ref, part_ref) = refs[:-8], refs[-8:]
    side = place[0]
    rows = zn.shape[0] // 2
    size = first.shape[0]
    z = own_rows(zn, side, size)
    outer, split, second = side_products(got[...], place[1], z, own_rows(zm, side, size), first[...], 2 * rows)
    part_ref[...] = part[...] + nn(split, halves_of(d_near[...]))
    new_ref[...] = kept(z + 0.5 * outer + 0.375 * second, pats, side, 2 * side, rows)


def far_blocks(place, pats, got, zm, zf, first, part, pay):
    side = place[0]
    width = zm.shape[0]
    rows = width // 2
    size = first.shape[0]
    z, mid = own_rows(zf, side, size), own_rows(zm, side, size)
    outer, split, second = side_products(got[...], place[2], z, mid, first[...], width)
    second_mid = part[...] + nn(split, halves_of(pay[width:]))
    far = kept(z + 0.5 * outer + 0.375 * second, pats, side, 2 - 2 * side, rows)
    return kept(mid + 0.5 * first[...] + 0.375 * second_mid, pats, side, 1, rows), far


def far_factor_kernel(place, pat_own, pat_oth, got, zm, zf, first, part, pay, pay_ref):
    width = zm.shape[0]
    middle, far = far_blocks(place, (pat_own, pat_oth), got, zm, zf, first, part, pay)
    pay_ref[:, :width] = middle
    pay_ref[:, width:] = far


def last_factor_kernel(place, pat_own, got, zm, zf, first, part, pay, near, out_ref):
    side = place[0]
    width = zm.shape[0]
    middle, far = far_blocks(place, (pat_own,), got, zm, zf, first, part, pay)
    low, high = ordered(side, near[...], far)
    out_ref[:, :width] = low
    out_ref[:, width:2 * width] = middle
    out_ref[:, 2 * width:] = high


def call(kernel, outs, scalars, arrays, flops=10**9):
    smem = pl.BlockSpec(memory_space=pltpu.SMEM)
    vmem = pl.BlockSpec(memory_space=pltpu.VMEM)
    shapes = [jax.ShapeDtypeStruct(s, F32) for s in outs]
    many = len(shapes) > 1
    return pl.pallas_call(
        kernel,
        out_shape=shapes if many else shapes[0],
        in_specs=[smem] * len(scalars) + [vmem] * len(arrays),
        out_specs=[vmem] * len(shapes) if many else vmem,
        cost_estimate=pl.CostEstimate(flops=flops, bytes_accessed=0, transcendentals=0),
        compiler_params=pltpu.CompilerParams(vmem_limit_bytes=16 * 2**20),
    )(*scalars, *arrays)


def per_device(intersect, half_factors, z_pattern):
    rows = intersect.shape[0]
    width = 2 * rows
    square = (width, width)
    count = lax.axis_size("blk")
    last = count - 1
    side = lax.axis_index("side")
    blk = lax.axis_index("blk")
    inner = jnp.stack([blk > 0, blk < last])
    place = jnp.stack([side, jnp.where(side == 0, inner[0], inner[1]), jnp.where(side == 0, inner[1], inner[0])])
    place = place.astype(jnp.int32)
    cycle = [(i, i + 1) for i in range(last)] + [(last, count + last)]
    cycle += [(count + i + 1, count + i) for i in range(last)] + [(count, 0)]

    def swap(value):
        return lax.ppermute(value, "side", [(0, 1), (1, 0)])

    def exchange(payload):
        got = lax.ppermute(payload, ("side", "blk"), cycle)
        return got, swap(got)

    s_oth, h_oth, p_oth = swap(intersect), swap(half_factors), swap(z_pattern)
    inputs = [intersect, s_oth, half_factors, h_oth]
    payload = call(start_kernel, [(width, 2 * width)], [place, p_oth], inputs)
    s_near, s_far = exchange(payload)
    z_near, z_far = s_near, s_far
    sn, sm, sf, zn, zm, zf, t_near, t_mid, t_far = call(first_local_kernel, [square] * 9, [place], inputs)
    for step in range(ITERS):
        final = step == ITERS - 1
        if step > 0:
            z_near, z_far = exchange(payload)
            t_near, t_mid, t_far = call(next_local_kernel, [square] * 3, [place], [sn, sm, sf, zm])
        mid, e_near, e_mid = call(
            near_image_kernel(step == 0), [square] * 3, [place], [s_near, z_near, sn, t_near, t_mid])
        mid, delta = call(
            far_image_kernel(step == 0), [square, (2 * width, width)], [place],
            [s_far, z_far, sf, zm, zf, t_far, mid, e_mid])
        d_own, d_oth = exchange(delta)
        band = (rows if final else width, width)
        pats = [z_pattern] if final else [z_pattern, p_oth]
        d_near, first, part = call(
            mid_first_kernel, [square, band, band], [place], [zn, zm, zf, e_near, mid, delta])
        near, part = call(near_factor_kernel, [band, band], [place] + pats, [d_own, zn, zm, first, part, d_near])
        rest = [d_oth, zm, zf, first, part, delta]
        if final:
            return call(last_factor_kernel, [(rows, 3 * width)], [place] + pats, rest + [near])
        payload = call(far_factor_kernel, [(width, 2 * width)], [place] + pats, rest)
        zn, zm, zf = near, payload[:, :width], payload[:, width:]


def solution(mesh):
    spec = P(("pair", "side", "blk"), None)
    return jax.shard_map(
        per_device,
        mesh=mesh,
        in_specs=(spec, spec, spec),
        out_specs=spec,
        check_vma=False,
    )
```

```python
import jax
import jax.numpy as jnp
from jax import lax
from jax.experimental import pallas as pl
from jax.experimental.pallas import tpu as pltpu
from jax.sharding import PartitionSpec as P


ITERS = 2
BF = jnp.bfloat16
F32 = jnp.float32


def halves_of(value):
    high = value.astype(BF)
    low = (value - high.astype(F32)).astype(BF)
    return high, low


def product(left, right, dims):
    (lh, ll), (rh, rl) = left, right

    def dot(a, b):
        return lax.dot_general(a, b, (dims, ((), ())), preferred_element_type=F32)

    return dot(lh, rh) + (dot(lh, rl) + dot(ll, rh))


def nn(left, right):
    return product(left, right, ((1,), (0,)))


def tn(left, right):
    return product(left, right, ((0,), (0,)))


def ordered(side, own, other):
    return jnp.where(side == 0, own, other), jnp.where(side == 0, other, own)


def block_diag(top, bottom):
    zero = jnp.zeros_like(top)
    return jnp.concatenate(
        [jnp.concatenate([top, zero], axis=1), jnp.concatenate([zero, bottom], axis=1)], axis=0
    )


def oriented(side, row, width):
    first, middle, final = [row[:, e * width:(e + 1) * width] for e in range(3)]
    near, far = ordered(side, first, final)
    return near, middle, far


def pack(value):
    rows = value.shape[0] // 2
    return jnp.concatenate([value[:rows, :rows], value[:rows, rows:], value[rows:, rows:]], axis=1)


def unpack(cells):
    rows = cells.shape[0]
    first, cross, final = [cells[:, e * rows:(e + 1) * rows] for e in range(3)]
    return jnp.concatenate(
        [jnp.concatenate([first, cross], axis=1), jnp.concatenate([cross.T, final], axis=1)], axis=0
    )


def stage_kernel(place, pat_own, s_own, h_own, s_out, h_out):
    width = s_out.shape[1]
    s_out[...] = s_own[:, width:2 * width]
    h_out[...] = h_own[...]


def start_kernel(place, pattern, s_own, s_oth, h_own, h_oth, pay_a, pay_b):
    side = place[0]
    rows = s_own.shape[0]
    width = 2 * rows
    top, bottom = ordered(side, s_own[...], s_oth[:, width:2 * width])
    pay_a[:, :width] = top
    pay_a[:, width:3 * rows] = bottom[:, rows:]
    top, bottom = ordered(side, h_own[...], h_oth[...])
    for e, part in enumerate((top, bottom)):
        _, middle, far = oriented(side, part, rows)
        pay_a[:, (3 + e) * rows:(4 + e) * rows] = far
        pay_b[:, e * rows:(e + 1) * rows] = middle


def image_local(s_row, z_mid, outs):
    near, middle, far = [halves_of(v) for v in s_row]
    z = halves_of(z_mid)
    outs[0][...] = tn(near, z)
    outs[1][...] = nn(middle, z)
    outs[2][...] = tn(far, z)


def first_local_kernel(place, s_own, s_oth, h_own, h_oth, sn, sm, sf, zn, zm, zf, tn_, tm, tf):
    side = place[0]
    rows = s_own.shape[0]
    width = 2 * rows
    s_all = jnp.concatenate(ordered(side, s_own[...], s_oth[...]), axis=0)
    s_row = oriented(side, s_all, width)
    top, bottom = ordered(side, h_own[...], h_oth[...])
    z_row = [block_diag(a, b) for a, b in zip(oriented(side, top, rows), oriented(side, bottom, rows))]
    for ref, v in zip((sn, sm, sf, zn, zm, zf), [*s_row, *z_row]):
        ref[...] = v
    image_local(s_row, z_row[1], (tn_, tm, tf))


def next_local_kernel(place, sn, sm, sf, zm, tn_, tm, tf):
    image_local((sn[...], sm[...], sf[...]), zm[...], (tn_, tm, tf))


def masked(ref, keep):
    return jnp.where(keep == 1, ref[...], 0.0)


def off_part(ref, keep, wide):
    got = masked(ref, keep)
    if wide:
        return halves_of(got)
    rows = got.shape[0]
    return halves_of(block_diag(got[:, 3 * rows:4 * rows], got[:, 4 * rows:]))


def diag_part(ref, keep, wide):
    got = masked(ref, keep)
    if wide:
        return halves_of(got)
    rows = got.shape[0]
    return halves_of(block_diag(got[:, :rows], got[:, rows:]))


def overlap_part(ref, keep):
    got = masked(ref, keep)
    return halves_of(unpack(got[:, :3 * got.shape[0]]))


def near_image_kernel(wide):
    def kernel(place, s_got, z_got, sn, t_near, t_mid, mid_ref, image_ref, e_mid):
        off = off_part(z_got, place[1], wide)
        image = nn(overlap_part(s_got, place[1]), off) + t_near[...]
        image_ref[...] = image
        mid_ref[...] = t_mid[...] + nn(halves_of(sn[...]), off)
        e_mid[...] = tn(off, halves_of(image))

    return kernel


def far_image_kernel(wide):
    def kernel(place, s_got, z_got, sf, zm, zf, t_far, mid_part, e_mid, mid_ref, image_ref, e_far, d_ref, pay_ref):
        width = t_far.shape[0]
        off = off_part(z_got, place[2], wide)
        middle = mid_part[...] + nn(halves_of(sf[...]), off)
        mid_ref[...] = middle
        middle = halves_of(middle)
        image = nn(overlap_part(s_got, place[2]), off) + t_far[...]
        image_ref[...] = image
        row_ids = lax.broadcasted_iota(jnp.int32, (width, width), 0)
        col_ids = lax.broadcasted_iota(jnp.int32, (width, width), 1)
        eye = (row_ids == col_ids).astype(F32)
        delta = eye - (e_mid[...] + tn(halves_of(zm[...]), middle) + tn(off, halves_of(image)))
        d_ref[...] = delta
        pay_ref[...] = pack(delta)
        e_far[...] = tn(halves_of(zf[...]), middle)

    return kernel


def near_delta_kernel(wide):
    def kernel(place, z_got, image, zn, mid, d_near):
        diag = diag_part(z_got, place[1], wide)
        d_near[...] = -(tn(halves_of(zn[...]), halves_of(mid[...])) + tn(diag, halves_of(image[...])))

    return kernel


def far_delta_kernel(wide):
    def kernel(place, z_got, image, e_far, d_far):
        diag = diag_part(z_got, place[2], wide)
        d_far[...] = -(e_far[...] + tn(diag, halves_of(image[...])))

    return kernel


def own_rows(ref, side, rows):
    if ref.shape[0] == rows:
        return ref[...]
    return jnp.where(side == 0, ref[:rows, :], ref[rows:, :])


def mid_first_kernel(place, zn, zm, zf, d_near, d_mid, d_far, first_ref, part_ref):
    side = place[0]
    rows = first_ref.shape[0]
    middle = halves_of(d_mid[...])
    first = nn(halves_of(own_rows(zn, side, rows)), halves_of(d_near[...]))
    first += nn(halves_of(own_rows(zm, side, rows)), middle)
    first += nn(halves_of(own_rows(zf, side, rows)), halves_of(d_far[...]))
    first_ref[...] = first
    part_ref[...] = nn(halves_of(first), middle)


def diag_kernel(place, d_own, d_oth, zn, zf, near_ref, far_ref, diag_near, diag_far):
    side = place[0]
    rows = near_ref.shape[0]
    for keep, got, z, ref, full in ((place[1], d_own, zn, near_ref, diag_near), (place[2], d_oth, zf, far_ref, diag_far)):
        diag = unpack(masked(got, keep))
        full[...] = diag
        ref[...] = nn(halves_of(own_rows(z, side, rows)), halves_of(diag))


def kept(values, pats, side, slot, rows):
    count = pats[0].shape[0]
    tile = rows // count
    both = values.shape[0] != rows
    bands = []
    for f in range(2 if both else 1):
        half = f if both else side
        for i in range(count):
            cells = []
            for q in range(2 * count):
                at = slot * 2 * count + q
                bit = jnp.where(side == f, pats[0][i, at], pats[1][i, at]) if both else pats[0][i, at]
                flag = jnp.logical_or(bit == 1, (2 + half) * count + i == at)
                top = (f * count + i) * tile
                cell = values[top:top + tile, q * tile:(q + 1) * tile]
                cells.append(jnp.where(flag, 1.0, 0.0) * cell)
            bands.append(jnp.concatenate(cells, axis=1))
    return jnp.concatenate(bands, axis=0) if len(bands) > 1 else bands[0]


def side_products(got, keep, diag, z_diag, z_mid, first):
    off = halves_of(masked(got, keep))
    outer = z_diag[...] + nn(halves_of(z_mid), off)
    split = halves_of(outer)
    second = nn(split, halves_of(diag[...])) + nn(halves_of(first[...]), off)
    return outer, split, second


def near_factor_kernel(place, *refs):
    pats, (got, diag, z_diag, zn, zm, first, part, d_near, new_ref, part_ref) = refs[:-10], refs[-10:]
    side = place[0]
    rows = zn.shape[0] // 2
    size = first.shape[0]
    outer, split, second = side_products(got, place[1], diag, z_diag, own_rows(zm, side, size), first)
    part_ref[...] = part[...] + nn(split, halves_of(d_near[...]))
    z = own_rows(zn, side, size)
    new_ref[...] = kept(z + 0.5 * outer + 0.375 * second, pats, side, 2 * side, rows)


def far_blocks(place, pats, got, diag, z_diag, zm, zf, first, part, d_far):
    side = place[0]
    rows = zm.shape[0] // 2
    size = first.shape[0]
    z, mid = own_rows(zf, side, size), own_rows(zm, side, size)
    outer, split, second = side_products(got, place[2], diag, z_diag, mid, first)
    second_mid = part[...] + nn(split, halves_of(d_far[...]))
    far = kept(z + 0.5 * outer + 0.375 * second, pats, side, 2 - 2 * side, rows)
    return kept(mid + 0.5 * first[...] + 0.375 * second_mid, pats, side, 1, rows), far


def far_factor_kernel(place, pat_own, pat_oth, *refs):
    refs[-2][...], refs[-1][...] = far_blocks(place, (pat_own, pat_oth), *refs[:-2])


def last_factor_kernel(place, pat_own, *refs):
    near, out_ref = refs[-2:]
    width = near.shape[1]
    middle, far = far_blocks(place, (pat_own,), *refs[:-2])
    low, high = ordered(place[0], near[...], far)
    out_ref[:, :width] = low
    out_ref[:, width:2 * width] = middle
    out_ref[:, 2 * width:] = high


def call(kernel, outs, scalars, arrays, flops=10**9):
    smem = pl.BlockSpec(memory_space=pltpu.SMEM)
    vmem = pl.BlockSpec(memory_space=pltpu.VMEM)
    shapes = [jax.ShapeDtypeStruct(s, F32) for s in outs]
    many = len(shapes) > 1
    return pl.pallas_call(
        kernel,
        out_shape=shapes if many else shapes[0],
        in_specs=[smem] * len(scalars) + [vmem] * len(arrays),
        out_specs=[vmem] * len(shapes) if many else vmem,
        cost_estimate=pl.CostEstimate(flops=flops, bytes_accessed=0, transcendentals=0),
        compiler_params=pltpu.CompilerParams(vmem_limit_bytes=16 * 2**20),
    )(*scalars, *arrays)


def per_device(intersect, half_factors, z_pattern):
    rows = intersect.shape[0]
    width = 2 * rows
    square = (width, width)
    count = lax.axis_size("blk")
    last = count - 1
    side = lax.axis_index("side")
    blk = lax.axis_index("blk")
    inner = jnp.stack([blk > 0, blk < last])
    place = jnp.stack([side, jnp.where(side == 0, inner[0], inner[1]), jnp.where(side == 0, inner[1], inner[0])])
    place = place.astype(jnp.int32)
    cycle = [(i, i + 1) for i in range(last)] + [(last, count + last)]
    cycle += [(count + i + 1, count + i) for i in range(last)] + [(count, 0)]

    def swap(value):
        return lax.ppermute(value, "side", [(0, 1), (1, 0)])

    def exchange(payload):
        got = lax.ppermute(payload, ("side", "blk"), cycle)
        return got, swap(got)

    s_oth, h_oth, p_oth = swap(intersect), swap(half_factors), swap(z_pattern)
    s_mid, h_own = call(stage_kernel, [(rows, width), (rows, 3 * rows)], [place, z_pattern], [intersect, half_factors])
    off, diag = call(start_kernel, [(rows, 5 * rows), (rows, width)], [place, p_oth], [s_mid, s_oth, h_own, h_oth])
    s_near, s_far = z_near, z_far = exchange(off)
    g_near, g_far = exchange(diag)
    sn, sm, sf, zn, zm, zf, t_near, t_mid, t_far = call(
        first_local_kernel, [square] * 9, [place], [intersect, s_oth, h_own, h_oth])
    for step in range(ITERS):
        final, wide = step == ITERS - 1, step > 0
        if wide:
            z_near, z_far = exchange(zf)
            g_near, g_far = exchange(zm)
            t_near, t_mid, t_far = call(next_local_kernel, [square] * 3, [place], [sn, sm, sf, zm])
        mid, i_near, e_mid = call(
            near_image_kernel(wide), [square] * 3, [place], [s_near, z_near, sn, t_near, t_mid])
        mid, i_far, e_far, d_mid, diag = call(
            far_image_kernel(wide), [square] * 4 + [(rows, 3 * rows)], [place],
            [s_far, z_far, sf, zm, zf, t_far, mid, e_mid])
        g_own, g_oth = exchange(diag)
        d_near = call(near_delta_kernel(wide), [square], [place], [g_near, i_near, zn, mid])
        d_far = call(far_delta_kernel(wide), [square], [place], [g_far, i_far, e_far])
        d_own, d_oth = exchange(d_far)
        band = (rows if final else width, width)
        pats = [z_pattern] if final else [z_pattern, p_oth]
        first, part = call(
            mid_first_kernel, [band, band], [place], [zn, zm, zf, d_near, d_mid, d_far])
        z_dn, z_df, diag_n, diag_f = call(
            diag_kernel, [band, band, square, square], [place], [g_own, g_oth, zn, zf])
        near, part = call(
            near_factor_kernel, [band, band], [place] + pats,
            [d_own, diag_n, z_dn, zn, zm, first, part, d_near])
        rest = [d_oth, diag_f, z_df, zm, zf, first, part, d_far]
        if final:
            return call(last_factor_kernel, [(rows, 3 * width)], [place] + pats, rest + [near])
        zm, zf = call(far_factor_kernel, [square, square], [place] + pats, rest)
        zn = near


def solution(mesh):
    spec = P(("pair", "side", "blk"), None)
    return jax.shard_map(
        per_device,
        mesh=mesh,
        in_specs=(spec, spec, spec),
        out_specs=spec,
        check_vma=False,
    )
```

```python
import jax
import jax.numpy as jnp
from jax import lax
from jax.experimental import pallas as pl
from jax.experimental.pallas import tpu as pltpu
from jax.sharding import PartitionSpec as P


ITERS = 2
BF = jnp.bfloat16
F32 = jnp.float32


def halves_of(value):
    high = value.astype(BF)
    low = (value - high.astype(F32)).astype(BF)
    return high, low


def product(left, right, dims):
    (lh, ll), (rh, rl) = left, right

    def dot(a, b):
        return lax.dot_general(a, b, (dims, ((), ())), preferred_element_type=F32)

    return dot(lh, rh) + (dot(lh, rl) + dot(ll, rh))


def nn(left, right):
    return product(left, right, ((1,), (0,)))


def tn(left, right):
    return product(left, right, ((0,), (0,)))


def ordered(side, own, other):
    return jnp.where(side == 0, own, other), jnp.where(side == 0, other, own)


def block_diag(top, bottom):
    zero = jnp.zeros_like(top)
    return jnp.concatenate(
        [jnp.concatenate([top, zero], axis=1), jnp.concatenate([zero, bottom], axis=1)], axis=0
    )


def oriented(side, row, width):
    first, middle, final = [row[:, e * width:(e + 1) * width] for e in range(3)]
    near, far = ordered(side, first, final)
    return near, middle, far


def pack(value):
    rows = value.shape[0] // 2
    return jnp.concatenate([value[:rows, :rows], value[:rows, rows:], value[rows:, rows:]], axis=1)


def unpack(cells):
    rows = cells.shape[0]
    first, cross, final = [cells[:, e * rows:(e + 1) * rows] for e in range(3)]
    return jnp.concatenate(
        [jnp.concatenate([first, cross], axis=1), jnp.concatenate([cross.T, final], axis=1)], axis=0
    )


def stage_kernel(place, s_own, h_own, s_out, h_out):
    width = s_out.shape[1]
    s_out[...] = s_own[:, width:2 * width]
    h_out[...] = h_own[...]


def start_kernel(place, pattern, s_own, s_oth, h_own, h_oth, pay_a, pay_b):
    side = place[0]
    rows = s_own.shape[0]
    width = 2 * rows
    top, bottom = ordered(side, s_own[...], s_oth[:, width:2 * width])
    pay_a[:, :width] = top
    pay_a[:, width:3 * rows] = bottom[:, rows:]
    top, bottom = ordered(side, h_own[...], h_oth[...])
    for e, part in enumerate((top, bottom)):
        _, middle, far = oriented(side, part, rows)
        pay_a[:, (3 + e) * rows:(4 + e) * rows] = far
        pay_b[:, e * rows:(e + 1) * rows] = middle


def image_local(s_row, z_mid, outs):
    near, middle, far = [halves_of(v) for v in s_row]
    z = halves_of(z_mid)
    outs[0][...] = tn(near, z)
    outs[1][...] = nn(middle, z)
    outs[2][...] = tn(far, z)


def first_local_kernel(place, pat_own, s_own, s_oth, h_own, h_oth, sn, sm, sf, zn, zm, zf, tn_, tm, tf):
    side = place[0]
    rows = s_own.shape[0]
    width = 2 * rows
    s_all = jnp.concatenate(ordered(side, s_own[...], s_oth[...]), axis=0)
    s_row = oriented(side, s_all, width)
    top, bottom = ordered(side, h_own[...], h_oth[...])
    z_row = [block_diag(a, b) for a, b in zip(oriented(side, top, rows), oriented(side, bottom, rows))]
    for ref, v in zip((sn, sm, sf, zn, zm, zf), [*s_row, *z_row]):
        ref[...] = v
    image_local(s_row, z_row[1], (tn_, tm, tf))


def next_local_kernel(place, sn, sm, sf, zm, tn_, tm, tf):
    image_local((sn[...], sm[...], sf[...]), zm[...], (tn_, tm, tf))


def masked(ref, keep):
    return jnp.where(keep == 1, ref[...], 0.0)


def off_part(ref, keep, wide):
    got = masked(ref, keep)
    if wide:
        return halves_of(got)
    rows = got.shape[0]
    return halves_of(block_diag(got[:, 3 * rows:4 * rows], got[:, 4 * rows:]))


def diag_part(ref, keep, wide):
    got = masked(ref, keep)
    if wide:
        return halves_of(got)
    rows = got.shape[0]
    return halves_of(block_diag(got[:, :rows], got[:, rows:]))


def overlap_part(ref, keep):
    got = masked(ref, keep)
    return halves_of(unpack(got[:, :3 * got.shape[0]]))


def near_image_kernel(wide):
    def kernel(place, s_got, z_got, sn, t_near, t_mid, mid_ref, image_ref, e_mid):
        off = off_part(z_got, place[1], wide)
        image = nn(overlap_part(s_got, place[1]), off) + t_near[...]
        image_ref[...] = image
        mid_ref[...] = t_mid[...] + nn(halves_of(sn[...]), off)
        e_mid[...] = tn(off, halves_of(image))

    return kernel


def far_image_kernel(wide):
    def kernel(place, s_got, z_got, sf, zm, zf, t_far, mid_part, e_mid, mid_ref, image_ref, e_far, d_ref, pay_ref):
        width = t_far.shape[0]
        off = off_part(z_got, place[2], wide)
        middle = mid_part[...] + nn(halves_of(sf[...]), off)
        mid_ref[...] = middle
        middle = halves_of(middle)
        image = nn(overlap_part(s_got, place[2]), off) + t_far[...]
        image_ref[...] = image
        row_ids = lax.broadcasted_iota(jnp.int32, (width, width), 0)
        col_ids = lax.broadcasted_iota(jnp.int32, (width, width), 1)
        eye = (row_ids == col_ids).astype(F32)
        delta = eye - (e_mid[...] + tn(halves_of(zm[...]), middle) + tn(off, halves_of(image)))
        d_ref[...] = delta
        pay_ref[...] = pack(delta)
        e_far[...] = tn(halves_of(zf[...]), middle)

    return kernel


def near_delta_kernel(wide):
    def kernel(place, z_got, image, zn, mid, d_near):
        diag = diag_part(z_got, place[1], wide)
        d_near[...] = -(tn(halves_of(zn[...]), halves_of(mid[...])) + tn(diag, halves_of(image[...])))

    return kernel


def far_delta_kernel(wide):
    def kernel(place, z_got, image, e_far, d_far):
        diag = diag_part(z_got, place[2], wide)
        d_far[...] = -(e_far[...] + tn(diag, halves_of(image[...])))

    return kernel


def own_rows(ref, side, rows):
    if ref.shape[0] == rows:
        return ref[...]
    return jnp.where(side == 0, ref[:rows, :], ref[rows:, :])


def mid_first_kernel(place, zn, zm, zf, d_near, d_mid, d_far, first_ref, part_ref):
    side = place[0]
    rows = first_ref.shape[0]
    middle = halves_of(d_mid[...])
    first = nn(halves_of(own_rows(zn, side, rows)), halves_of(d_near[...]))
    first += nn(halves_of(own_rows(zm, side, rows)), middle)
    first += nn(halves_of(own_rows(zf, side, rows)), halves_of(d_far[...]))
    first_ref[...] = first
    part_ref[...] = nn(halves_of(first), middle)


def diag_kernel(place, d_own, d_oth, zn, zf, near_ref, far_ref, diag_near, diag_far):
    side = place[0]
    rows = near_ref.shape[0]
    for keep, got, z, ref, full in ((place[1], d_own, zn, near_ref, diag_near), (place[2], d_oth, zf, far_ref, diag_far)):
        diag = unpack(masked(got, keep))
        full[...] = diag
        ref[...] = nn(halves_of(own_rows(z, side, rows)), halves_of(diag))


def kept(values, pats, side, slot, rows):
    count = pats[0].shape[0]
    tile = rows // count
    both = values.shape[0] != rows
    bands = []
    for f in range(2 if both else 1):
        half = f if both else side
        for i in range(count):
            cells = []
            for q in range(2 * count):
                at = slot * 2 * count + q
                bit = jnp.where(side == f, pats[0][i, at], pats[1][i, at]) if both else pats[0][i, at]
                flag = jnp.logical_or(bit == 1, (2 + half) * count + i == at)
                top = (f * count + i) * tile
                cell = values[top:top + tile, q * tile:(q + 1) * tile]
                cells.append(jnp.where(flag, 1.0, 0.0) * cell)
            bands.append(jnp.concatenate(cells, axis=1))
    return jnp.concatenate(bands, axis=0) if len(bands) > 1 else bands[0]


def side_products(got, keep, diag, z_diag, z_mid, first):
    off = halves_of(masked(got, keep))
    outer = z_diag[...] + nn(halves_of(z_mid), off)
    split = halves_of(outer)
    second = nn(split, halves_of(diag[...])) + nn(halves_of(first[...]), off)
    return outer, split, second


def near_factor_kernel(place, *refs):
    pats, (got, diag, z_diag, zn, zm, first, part, d_near, new_ref, part_ref) = refs[:-10], refs[-10:]
    side = place[0]
    rows = zn.shape[0] // 2
    size = first.shape[0]
    outer, split, second = side_products(got, place[1], diag, z_diag, own_rows(zm, side, size), first)
    part_ref[...] = part[...] + nn(split, halves_of(d_near[...]))
    z = own_rows(zn, side, size)
    new_ref[...] = kept(z + 0.5 * outer + 0.375 * second, pats, side, 2 * side, rows)


def far_blocks(place, pats, got, diag, z_diag, zm, zf, first, part, d_far):
    side = place[0]
    rows = zm.shape[0] // 2
    size = first.shape[0]
    z, mid = own_rows(zf, side, size), own_rows(zm, side, size)
    outer, split, second = side_products(got, place[2], diag, z_diag, mid, first)
    second_mid = part[...] + nn(split, halves_of(d_far[...]))
    far = kept(z + 0.5 * outer + 0.375 * second, pats, side, 2 - 2 * side, rows)
    return kept(mid + 0.5 * first[...] + 0.375 * second_mid, pats, side, 1, rows), far


def far_factor_kernel(place, pat_own, pat_oth, *refs):
    refs[-2][...], refs[-1][...] = far_blocks(place, (pat_own, pat_oth), *refs[:-2])


def last_factor_kernel(place, pat_own, *refs):
    near, out_ref = refs[-2:]
    width = near.shape[1]
    middle, far = far_blocks(place, (pat_own,), *refs[:-2])
    low, high = ordered(place[0], near[...], far)
    out_ref[:, :width] = low
    out_ref[:, width:2 * width] = middle
    out_ref[:, 2 * width:] = high


def call(kernel, outs, scalars, arrays, flops=10**9):
    smem = pl.BlockSpec(memory_space=pltpu.SMEM)
    vmem = pl.BlockSpec(memory_space=pltpu.VMEM)
    shapes = [jax.ShapeDtypeStruct(s, F32) for s in outs]
    many = len(shapes) > 1
    return pl.pallas_call(
        kernel,
        out_shape=shapes if many else shapes[0],
        in_specs=[smem] * len(scalars) + [vmem] * len(arrays),
        out_specs=[vmem] * len(shapes) if many else vmem,
        cost_estimate=pl.CostEstimate(flops=flops, bytes_accessed=0, transcendentals=0),
        compiler_params=pltpu.CompilerParams(vmem_limit_bytes=16 * 2**20),
    )(*scalars, *arrays)


def per_device(intersect, half_factors, z_pattern):
    rows = intersect.shape[0]
    width = 2 * rows
    square = (width, width)
    count = lax.axis_size("blk")
    last = count - 1
    side = lax.axis_index("side")
    blk = lax.axis_index("blk")
    inner = jnp.stack([blk > 0, blk < last])
    place = jnp.stack([side, jnp.where(side == 0, inner[0], inner[1]), jnp.where(side == 0, inner[1], inner[0])])
    place = place.astype(jnp.int32)
    cycle = [(i, i + 1) for i in range(last)] + [(last, count + last)]
    cycle += [(count + i + 1, count + i) for i in range(last)] + [(count, 0)]

    def swap(value):
        return lax.ppermute(value, "side", [(0, 1), (1, 0)])

    def exchange(payload):
        got = lax.ppermute(payload, ("side", "blk"), cycle)
        return got, swap(got)

    s_oth, h_oth, p_oth = swap(intersect), swap(half_factors), swap(z_pattern)
    s_mid, h_own = call(stage_kernel, [(rows, width), (rows, 3 * rows)], [place], [intersect, half_factors])
    off, diag = call(start_kernel, [(rows, 5 * rows), (rows, width)], [place, p_oth], [s_mid, s_oth, h_own, h_oth])
    s_near, s_far = z_near, z_far = exchange(off)
    g_near, g_far = exchange(diag)
    sn, sm, sf, zn, zm, zf, t_near, t_mid, t_far = call(
        first_local_kernel, [square] * 9, [place, z_pattern], [intersect, s_oth, h_own, h_oth])
    for step in range(ITERS):
        final, wide = step == ITERS - 1, step > 0
        if wide:
            z_near, z_far = exchange(zf)
            g_near, g_far = exchange(zm)
            t_near, t_mid, t_far = call(next_local_kernel, [square] * 3, [place], [sn, sm, sf, zm])
        mid, i_near, e_mid = call(
            near_image_kernel(wide), [square] * 3, [place], [s_near, z_near, sn, t_near, t_mid])
        mid, i_far, e_far, d_mid, diag = call(
            far_image_kernel(wide), [square] * 4 + [(rows, 3 * rows)], [place],
            [s_far, z_far, sf, zm, zf, t_far, mid, e_mid])
        g_own, g_oth = exchange(diag)
        d_near = call(near_delta_kernel(wide), [square], [place], [g_near, i_near, zn, mid])
        d_far = call(far_delta_kernel(wide), [square], [place], [g_far, i_far, e_far])
        d_own, d_oth = exchange(d_far)
        band = (rows if final else width, width)
        pats = [z_pattern] if final else [z_pattern, p_oth]
        first, part = call(
            mid_first_kernel, [band, band], [place], [zn, zm, zf, d_near, d_mid, d_far])
        z_dn, z_df, diag_n, diag_f = call(
            diag_kernel, [band, band, square, square], [place], [g_own, g_oth, zn, zf])
        near, part = call(
            near_factor_kernel, [band, band], [place] + pats,
            [d_own, diag_n, z_dn, zn, zm, first, part, d_near])
        rest = [d_oth, diag_f, z_df, zm, zf, first, part, d_far]
        if final:
            return call(last_factor_kernel, [(rows, 3 * width)], [place] + pats, rest + [near])
        zm, zf = call(far_factor_kernel, [square, square], [place] + pats, rest)
        zn = near


def solution(mesh):
    spec = P(("pair", "side", "blk"), None)
    return jax.shard_map(
        per_device,
        mesh=mesh,
        in_specs=(spec, spec, spec),
        out_specs=spec,
        check_vma=False,
    )
```
